32 devices in a mesh: member: 2 (over x), tm: 8 (over z, y), lat: 2 (over core).
Axes of the slice: x: 2, y: 2, z: 4, core: 2. Of those that a mesh axis runs over, the one named last changes fastest.
Arguments:
- increments: float32 [16, 4, 8, 128, 256], P(('member', 'tm'), None, None, 'lat'), parts along dimension 0, may hold values from -6 to 6
- wind_lat: float32 [16, 128, 256], P('member', 'lat'), parts along dimension 0, may hold values from -1 to 1
- wind_lon: float32 [16, 128, 256], P('member', 'lat'), parts along dimension 0, may hold values from -1 to 1
- boundary: int32 [16, 128, 256], P('member', 'lat'), parts along dimension 0, may hold values 0 or 1
- coupling: float32 [4, 4], replicated, may hold values from -1.5 to 1.5
- precision_time: float32 [8, 8], replicated, as said below
Outputs:
- gradient: float32 [16, 4, 8, 128, 256], P(('member', 'tm'), None, None, 'lat'), parts along dimension 0
The draws below stay inside these ranges and needn't reach their ends.
There are 2 independent parts, one for each index of `member`. The reference program is written for one: setup_inputs(seed, part) draws one part's arguments, and reference() takes and returns one part's arrays. A program takes and returns all parts, laid end to end along the dimension named above; an argument that names none is the same for every part. Nothing has to cross between parts.
Inputs may be any that keep to these rules, and one draw needn't show every extreme that they name: `precision_time`: symmetric.
All inputs are finite; a program needn't handle non-finite values. No bound on the sum of `boundary` on one device may be relied on, other than what follows from the above.
Results may differ from the reference program's by a relative error of at most 0.0001.
Values sent between devices are 32-bit elements; how exact they have to be, the bound alone decides.
No kernel may reach another device: no remote copies, remote signals or barrier semaphores. Data moves between devices by JAX's collectives and lax.ppermute only.
A program may use at most 128 MiB of HBM per device.

```python
import jax
import jax.numpy as jnp
from jax import lax

VARS = 4
LEV = 8
NLON = 256
STEPS = 4
NWIN = 8
NLAT = 128


def draw_precision_time(key, part):
    first_key, second_key = jax.random.split(jax.random.fold_in(key, 11))
    random_part = jax.random.normal(first_key, (NWIN, NWIN), jnp.float32) * (0.6 / NWIN ** 0.5)
    symmetric = 0.5 * (random_part + random_part.T)
    diagonal = jax.random.uniform(second_key, (NWIN,), jnp.float32, 1.0, 2.5)
    return symmetric + jnp.diag(diagonal)


def place_ends(array, own_key, least, top_value):
    longest = array.shape.index(max(array.shape))
    spots = []
    for shift in (0, 1):
        where = [jax.random.randint(jax.random.fold_in(own_key, axis), (), 0, length) for axis, length in enumerate(array.shape)]
        where[longest] = (where[longest] + shift) % array.shape[longest]
        spots.append(tuple(where))
    return array.at[spots[0]].set(least).at[spots[1]].set(top_value)


def level_of(stream_key, shape, cuts, low, top_value):
    def one(dim, parts):
        draws = jax.random.uniform(jax.random.fold_in(jax.random.fold_in(stream_key, 6), dim), (parts,), jnp.float32, low / len(cuts), top_value / len(cuts))
        return jnp.repeat(jnp.exp(draws), shape[dim] // parts).reshape((-1,) + (1,) * (len(shape) - dim - 1))

    gain = one(*cuts[0])
    for cut in cuts[1:]:
        gain = gain * one(*cut)
    return gain


def normal_values(stream_key, extent, scale, bound, cuts=(), kind=jnp.bfloat16):
    entries = scale * jax.random.normal(stream_key, extent, jnp.float32)
    if cuts:
        entries = entries * level_of(stream_key, extent, cuts, -0.22, 0.18)
    return jnp.clip(entries, -bound, bound).astype(kind)


def setup_inputs(seed: int = 0, part: int = 0) -> dict:
    key_of = jax.random.split(jax.random.key(seed), 7)
    part_splits = jax.random.split(jax.random.fold_in(key_of[6], part), 7)
    return {
        "increments": normal_values(part_splits[0], (NWIN, VARS, LEV, NLAT, NLON), 1.0, 6.0, ((0, 8), (3, 2)), jnp.float32),
        "wind_lat": jnp.clip(jax.random.uniform(part_splits[1], (LEV, NLAT, NLON), jnp.float32, -1.0, 1.0) * level_of(part_splits[1], (LEV, NLAT, NLON), ((1, 2),), -0.4, 0.0), -1.0, 1.0),
        "wind_lon": jnp.clip(jax.random.uniform(part_splits[2], (LEV, NLAT, NLON), jnp.float32, -1.0, 1.0) * level_of(part_splits[2], (LEV, NLAT, NLON), ((1, 2),), -0.4, 0.0), -1.0, 1.0),
        "boundary": place_ends((jax.random.randint(part_splits[3], (LEV, NLAT, NLON), 0, 4) < 1).astype(jnp.int32), jax.random.fold_in(part_splits[3], 1), 0, 1),
        "coupling": normal_values(key_of[4], (VARS, VARS), 0.3, 1.5, (), jnp.float32),
        "precision_time": draw_precision_time(jax.random.fold_in(key_of[6], 71), part),
    }


KAPPA = 0.2
RELAX = 0.5
DT = 0.4
HIGHEST = lax.Precision.HIGHEST


def forward_tendency(padded, coefficients, coupling):
    centre = padded[..., 1:-1, 1:-1]
    wind_north = coefficients[0][None, None, :, 1:-1, 1:-1]
    wind_east = coefficients[1][None, None, :, 1:-1, 1:-1]
    held = coefficients[2][None, None, :, 1:-1, 1:-1]
    northern = padded[..., 2:, 1:-1]
    southern = padded[..., :-2, 1:-1]
    eastern = padded[..., 1:-1, 2:]
    western = padded[..., 1:-1, :-2]
    mixed = jnp.einsum("vu,wulrn->wvlrn", coupling, centre, precision=HIGHEST)
    drift = -wind_north * (northern - southern) * 0.5 - wind_east * (eastern - western) * 0.5
    spread = KAPPA * (northern + southern + eastern + western - 4.0 * centre)
    return (1.0 - held) * (drift + spread + mixed) - RELAX * held * centre


def adjoint_tendency(padded, coefficients, coupling):
    wind_north = coefficients[0][None, None]
    wind_east = coefficients[1][None, None]
    held = coefficients[2][None, None]
    weighted = (1.0 - held) * padded
    along_north = wind_north * weighted
    along_east = wind_east * weighted
    centre = weighted[..., 1:-1, 1:-1]
    drift = (along_north[..., 2:, 1:-1] - along_north[..., :-2, 1:-1]) * 0.5
    drift = drift + (along_east[..., 1:-1, 2:] - along_east[..., 1:-1, :-2]) * 0.5
    spread = KAPPA * (weighted[..., 2:, 1:-1] + weighted[..., :-2, 1:-1] + weighted[..., 1:-1, 2:] + weighted[..., 1:-1, :-2] - 4.0 * centre)
    mixed = jnp.einsum("uv,wulrn->wvlrn", coupling, centre, precision=HIGHEST)
    return drift + spread + mixed - RELAX * held[..., 1:-1, 1:-1] * padded[..., 1:-1, 1:-1]


def surround(field):
    return jnp.pad(field, ((0, 0), (0, 0), (0, 0), (1, 1), (1, 1)))


def advance(field, tendency, coefficients, coupling):
    first = tendency(surround(field), coefficients, coupling)
    middle = field + DT * first
    second = tendency(surround(middle), coefficients, coupling)
    return field + 0.5 * DT * (first + second)


def reference(increments, wind_lat, wind_lon, boundary, coupling, precision_time):
    coefficients = jnp.stack([wind_lat, wind_lon, boundary.astype(jnp.float32)])
    coefficients = jnp.pad(coefficients, ((0, 0), (0, 0), (1, 1), (1, 1)))
    current = increments
    for repeat in range(STEPS):
        current = advance(current, forward_tendency, coefficients, coupling)
    zeroed = jnp.zeros_like(current[:1])
    defects = increments - jnp.concatenate([zeroed, current[:-1]], 0)
    weighted = jnp.einsum("kj,jvlrn->kvlrn", precision_time, defects, precision=HIGHEST)
    backward = weighted
    for repeat in range(STEPS):
        backward = advance(backward, adjoint_tendency, coefficients, coupling)
    return weighted - jnp.concatenate([backward[1:], zeroed], 0)
```

```python
import functools

import jax
import jax.numpy as jnp
from jax import lax
from jax.experimental import pallas as pl
from jax.experimental.pallas import tpu as pltpu
from jax.sharding import PartitionSpec as P

STEPS = 4


KAPPA = 0.2
RELAX = 0.5
DT = 0.4
HIGHEST = lax.Precision.HIGHEST
LANES = 128
ROWS = 8
SCALE = 0.5**STEPS


def rolled(values, shift):
    return [pltpu.roll(value, shift, axis=1) for value in values]


def east_of(values, lane):
    moved = rolled(values, LANES - 1)
    count = len(values)
    return [
        jnp.where(lane == LANES - 1, moved[(part + 1) % count], moved[part])
        for part in range(count)
    ]


def west_of(values, lane):
    moved = rolled(values, 1)
    count = len(values)
    return [jnp.where(lane == 0, moved[part - 1], moved[part]) for part in range(count)]


def apply_operator(source, target, coef, coupling, add):
    variables, parts = source.shape[0], source.shape[1]
    tiles = coef.shape[2] // ROWS
    lane = lax.broadcasted_iota(jnp.int32, (ROWS, LANES), 1)
    for tile in range(tiles):
        at = ROWS * (tile + 1)
        here = slice(at, at + ROWS)
        centre = [[source[v, p, here, :] for p in range(parts)] for v in range(variables)]
        east = [east_of(values, lane) for values in centre]
        west = [west_of(values, lane) for values in centre]
        for p in range(parts):
            rows = slice(ROWS * tile, ROWS * (tile + 1))
            to_north, to_south, to_east, to_west = (coef[i, p, rows, :] for i in range(4))
            held = coef[4, p, rows, :] != 0.0
            for v in range(variables):
                mixed = coupling[v][0] * centre[0][p]
                for u in range(1, variables):
                    mixed = mixed + coupling[v][u] * centre[u][p]
                local = jnp.where(held, (1.0 - DT * RELAX) * centre[v][p], mixed)
                lat = (
                    to_north * source[v, p, at + 1 : at + 1 + ROWS, :]
                    + to_south * source[v, p, at - 1 : at - 1 + ROWS, :]
                )
                lon = to_east * east[v][p] + to_west * west[v][p]
                value = local + (lat + lon)
                if add:
                    value = value + target[v, p, here, :]
                target[v, p, here, :] = value


def clear_rims(*buffers):
    for buffer in buffers:
        height = buffer.shape[2]
        rim = jnp.zeros((ROWS, LANES), jnp.float32)
        for v in range(buffer.shape[0]):
            for p in range(buffer.shape[1]):
                buffer[v, p, 0:ROWS, :] = rim
                buffer[v, p, height - ROWS : height, :] = rim


def run_window(state, middle, coef, coupling):
    def step(_, carry):
        apply_operator(state, middle, coef, coupling, False)
        apply_operator(middle, state, coef, coupling, True)
        return carry

    lax.fori_loop(0, STEPS, step, 0)


def aligned(start):
    return pl.ds(pl.multiple_of(start, ROWS), ROWS)


def prepare_kernel(side_ref, own, halo, forward, adjoint, joined, kept):
    side = side_ref[0]
    reach, height = halo.shape[1], own.shape[1]
    parts = forward.shape[1]
    lane = lax.broadcasted_iota(jnp.int32, (ROWS, LANES), 1)
    for i in range(3):
        for p in range(parts):
            lanes = slice(p * LANES, (p + 1) * LANES)
            for t in range(height // ROWS):
                joined[i, p, aligned(reach * side + ROWS * t), :] = own[
                    i, ROWS * t : ROWS * (t + 1), lanes
                ]
            for t in range(reach // ROWS):
                joined[i, p, aligned(height * (1 - side) + ROWS * t), :] = halo[
                    i, ROWS * t : ROWS * (t + 1), lanes
                ]
    clear_rims(kept)
    tiles = (height + reach) // ROWS
    for t in range(tiles):
        rows = slice(ROWS * t, ROWS * (t + 1))
        here = slice(ROWS * (t + 1), ROWS * (t + 2))
        for p in range(parts):
            north, east, held = (joined[i, p, rows, :] for i in range(3))
            free = DT * (1.0 - held)
            values = [
                free * (KAPPA - 0.5 * north),
                free * (KAPPA + 0.5 * north),
                free * (KAPPA - 0.5 * east),
                free * (KAPPA + 0.5 * east),
            ]
            if p == parts - 1:
                values[2] = jnp.where(lane == LANES - 1, 0.0, values[2])
            if p == 0:
                values[3] = jnp.where(lane == 0, 0.0, values[3])
            for i, value in enumerate(values + [held]):
                forward[i, p, rows, :] = value
            for i in range(4):
                kept[i, p, here, :] = values[i]
    for t in range(tiles):
        rows = slice(ROWS * t, ROWS * (t + 1))
        at = ROWS * (t + 1)
        here = slice(at, at + ROWS)
        from_east = east_of([kept[3, p, here, :] for p in range(parts)], lane)
        from_west = west_of([kept[2, p, here, :] for p in range(parts)], lane)
        for p in range(parts):
            joined[0, p, rows, :] = kept[1, p, at + 1 : at + 1 + ROWS, :]
            joined[1, p, rows, :] = kept[0, p, at - 1 : at - 1 + ROWS, :]
            joined[3, p, rows, :] = from_east[p]
            joined[4, p, rows, :] = from_west[p]
    for t in range(adjoint.shape[2] // ROWS):
        rows = slice(ROWS * t, ROWS * (t + 1))
        at = aligned(reach // 2 * side + ROWS * t)
        for p in range(parts):
            for i, j in enumerate((0, 1, 3, 4, 2)):
                adjoint[i, p, rows, :] = joined[j, p, at, :]


def prepare(side, own, halo):
    fields, height, width = own.shape
    reach = halo.shape[1]
    parts = width // LANES
    vmem = pl.BlockSpec(memory_space=pltpu.VMEM)
    return pl.pallas_call(
        prepare_kernel,
        out_shape=(
            jax.ShapeDtypeStruct((5, parts, height + reach, LANES), jnp.float32),
            jax.ShapeDtypeStruct((5, parts, height + reach // 2, LANES), jnp.float32),
        ),
        in_specs=[pl.BlockSpec(memory_space=pltpu.SMEM), vmem, vmem],
        out_specs=(vmem, vmem),
        scratch_shapes=[
            pltpu.VMEM((5, parts, height + reach, LANES), jnp.float32),
            pltpu.VMEM((4, parts, height + reach + 2 * ROWS, LANES), jnp.float32),
        ],
        compiler_params=pltpu.CompilerParams(vmem_limit_bytes=16 * 2**20),
        cost_estimate=pl.CostEstimate(flops=2**20, bytes_accessed=2**20, transcendentals=0),
        name="prepare",
    )(side, own, halo)


def forward_kernel(count, first, side_ref, scalars, weights, coef, halo, *rest):
    pieces, rest = rest[:count], rest[count:]
    if first:
        total, state, middle, initial = rest
        before = None
    else:
        before, total, state, middle, initial = rest
    side = side_ref[0]
    variables, height = pieces[0].shape[0], pieces[0].shape[1]
    reach = halo.shape[2]
    parts = coef.shape[1]
    windows, inner = total.shape[0], total.shape[3]
    coupling = [[scalars[v, u] for u in range(variables)] for v in range(variables)]
    clear_rims(state, middle)
    for s, piece in enumerate(pieces):
        for v in range(variables):
            for p in range(parts):
                lanes = slice(p * LANES, (p + 1) * LANES)
                for t in range(height // ROWS):
                    state[v, p, aligned(ROWS + reach * side + ROWS * t), :] = piece[
                        v, ROWS * t : ROWS * (t + 1), lanes
                    ]
                for t in range(reach // ROWS):
                    state[v, p, aligned(ROWS + height * (1 - side) + ROWS * t), :] = halo[
                        s, v, ROWS * t : ROWS * (t + 1), lanes
                    ]
        for v in range(variables):
            for p in range(parts):
                for t in range(inner // ROWS):
                    initial[v, p, ROWS * t : ROWS * (t + 1), :] = state[
                        v, p, aligned(ROWS + reach // 2 * side + ROWS * t), :
                    ]
        run_window(state, middle, coef, coupling)
        of_initial = [weights[0, k, s] for k in range(windows)]
        of_final = [weights[1, k, s] for k in range(windows)]
        base = None if first and s == 0 else (total if first or s else before)

        def accumulate(v, carry):
            for p in range(parts):
                for t in range(inner // ROWS):
                    rows = slice(ROWS * t, ROWS * (t + 1))
                    start = initial[v, p, rows, :]
                    end = state[v, p, aligned(ROWS + reach // 2 * side + ROWS * t), :]
                    for k in range(windows):
                        value = of_initial[k] * start + of_final[k] * end
                        if base is not None:
                            value = base[k, v, p, rows, :] + value
                        total[k, v, p, rows, :] = value
            return carry

        lax.fori_loop(0, variables, accumulate, 0)


def forward(side, scalars, weights, coef, halo, pieces, before):
    count = len(pieces)
    variables, height, width = pieces[0].shape
    parts = width // LANES
    reach = halo.shape[2]
    windows = weights.shape[1]
    first = before is None
    inner = height + reach // 2
    vmem = pl.BlockSpec(memory_space=pltpu.VMEM)
    smem = pl.BlockSpec(memory_space=pltpu.SMEM)
    buffer = pltpu.VMEM((variables, parts, height + reach + 2 * ROWS, LANES), jnp.float32)
    arguments = [side, scalars, weights, coef, halo, *pieces] + ([] if first else [before])
    cells = count * variables * (height + reach) * width
    return pl.pallas_call(
        functools.partial(forward_kernel, count, first),
        out_shape=jax.ShapeDtypeStruct((windows, variables, parts, inner, LANES), jnp.float32),
        in_specs=[smem] * 3 + [vmem] * (len(arguments) - 3),
        out_specs=vmem,
        scratch_shapes=[
            buffer,
            buffer,
            pltpu.VMEM((variables, parts, inner, LANES), jnp.float32),
        ],
        input_output_aliases={} if first else {len(arguments) - 1: 0},
        compiler_params=pltpu.CompilerParams(vmem_limit_bytes=16 * 2**20),
        cost_estimate=pl.CostEstimate(
            flops=cells * 2 * STEPS * 20, bytes_accessed=4 * cells, transcendentals=0
        ),
        name="forward",
    )(*arguments)


def adjoint_kernel(count, numbers, scalars, coef, total, *rest):
    outs, (state, middle) = rest[:count], rest[count:]
    side = numbers[0]
    windows, variables, parts, inner = total.shape[:4]
    height = outs[0].shape[1]
    margin = inner - height
    coupling = [[scalars[u, v] for u in range(variables)] for v in range(variables)]
    clear_rims(state, middle)
    for s, out in enumerate(outs):
        window = numbers[1 + s]
        later = jnp.minimum(window + 1, windows - 1)
        present = window + 1 < windows
        for v in range(variables):
            for p in range(parts):
                for t in range(inner // ROWS):
                    value = total[later, v, p, ROWS * t : ROWS * (t + 1), :]
                    state[v, p, ROWS * (t + 1) : ROWS * (t + 2), :] = jnp.where(
                        present, value, 0.0
                    )
        run_window(state, middle, coef, coupling)
        for v in range(variables):
            for p in range(parts):
                for t in range(height // ROWS):
                    mine = total[window, v, p, aligned(margin * side + ROWS * t), :]
                    back = state[v, p, aligned(ROWS + margin * side + ROWS * t), :]
                    out[v, ROWS * t : ROWS * (t + 1), p * LANES : (p + 1) * LANES] = (
                        mine - SCALE * back
                    )


def adjoint(numbers, scalars, coef, total, count, height):
    windows, variables, parts, inner = total.shape[:4]
    vmem = pl.BlockSpec(memory_space=pltpu.VMEM)
    smem = pl.BlockSpec(memory_space=pltpu.SMEM)
    buffer = pltpu.VMEM((variables, parts, inner + 2 * ROWS, LANES), jnp.float32)
    shape = jax.ShapeDtypeStruct((variables, height, parts * LANES), jnp.float32)
    cells = count * variables * inner * parts * LANES
    return pl.pallas_call(
        functools.partial(adjoint_kernel, count),
        out_shape=(shape,) * count,
        in_specs=[smem, smem, vmem, vmem],
        out_specs=(vmem,) * count,
        scratch_shapes=[buffer, buffer],
        compiler_params=pltpu.CompilerParams(vmem_limit_bytes=16 * 2**20),
        cost_estimate=pl.CostEstimate(
            flops=cells * 2 * STEPS * 20, bytes_accessed=4 * cells, transcendentals=0
        ),
        name="adjoint",
    )(numbers, scalars, coef, total)


def groups_of(windows):
    half = windows // 2
    crossing = list(range(half, windows))
    near = list(range(1, half))
    return crossing, near


def by_level(increments, wind_lat, wind_lon, boundary, coupling, precision_time):
    windows = lax.axis_size("tm")
    me = lax.axis_index("tm")
    side = lax.axis_index("lat")
    height = increments.shape[3]
    reach = 4 * STEPS
    seam = (1 - side) * (height - reach)
    field = increments[0]
    sides = jnp.reshape(side, (1,)).astype(jnp.int32)
    other_core = [(0, 1), (1, 0)]

    def level_of(array, index, dim):
        return lax.dynamic_index_in_dim(array, index, dim, keepdims=False)

    def swapped(value, mask):
        return lax.ppermute(value, "tm", [(i, i ^ mask) for i in range(windows)])

    def seam_rows(value):
        return lax.dynamic_slice_in_dim(value, seam, reach, axis=value.ndim - 2)

    crossing, near = groups_of(windows)
    pieces = {0: level_of(field, me, 1)}
    for mask in crossing + near:
        pieces[mask] = swapped(level_of(field, me ^ mask, 1), mask)

    own = jnp.stack(
        [
            level_of(wind_lat, me, 0),
            level_of(wind_lon, me, 0),
            level_of(boundary, me, 0).astype(jnp.float32),
        ]
    )
    beyond = lax.ppermute(seam_rows(own), "lat", other_core)
    coef_forward, coef_adjoint = prepare(sides, own, beyond)

    factor = jnp.float32(1.0 - 4.0 * KAPPA * DT)
    scalars = DT * coupling + factor * jnp.eye(coupling.shape[0], dtype=jnp.float32)
    shifted = jnp.concatenate(
        [precision_time[:, 1:], jnp.zeros_like(precision_time[:, :1])], axis=1
    )
    tables = jnp.stack([precision_time, -SCALE * shifted])
    order = me ^ jnp.arange(windows, dtype=jnp.int32)
    tables = jnp.take(tables, order, axis=2)

    total = None
    for group in FORWARD_GROUPS(crossing, near):
        members = [pieces[mask] for mask in group]
        halo = lax.ppermute(jnp.stack([seam_rows(m) for m in members]), "lat", other_core)
        weights = jnp.stack([tables[:, :, mask] for mask in group], axis=2)
        total = forward(sides, scalars, weights, coef_forward, halo, members, total)

    gradient = jnp.zeros_like(field)
    for group in ADJOINT_GROUPS(crossing, near):
        numbers = jnp.concatenate([sides, jnp.stack([order[mask] for mask in group])])
        results = adjoint(numbers, scalars, coef_adjoint, total, len(group), height)
        for mask, result in zip(group, results):
            if mask:
                result = swapped(result, mask)
            gradient = lax.dynamic_update_slice(
                gradient, result[:, None], (0, me ^ mask, 0, 0)
            )
    return gradient[None]


def FORWARD_GROUPS(crossing, near):
    return [[0]] + [near] + [[mask] for mask in crossing]


def ADJOINT_GROUPS(crossing, near):
    return [[mask] for mask in crossing] + [[mask] for mask in near] + [[0]]


def extended_2(block, sides, width):
    for axis, dim in sides:
        count = lax.axis_size(axis)
        forward = [(i, i + 1) for i in range(count - 1)]
        backward = [(target, source) for source, target in forward]
        low = lax.ppermute(
            lax.slice_in_dim(block, block.shape[dim] - width, None, axis=dim), axis, forward
        )
        high = lax.ppermute(lax.slice_in_dim(block, 0, width, axis=dim), axis, backward)
        block = jnp.concatenate([low, block, high], axis=dim)
    return block


def from_behind(value, axis, steps):
    count = lax.axis_size(axis)
    initial, last = (max(0, -steps), min(count, count - steps))
    return lax.ppermute(value, axis, [(source, source + steps) for source in range(initial, last)])


def forward_tendency(padded, coefficients, coupling):
    centre = padded[..., 1:-1, 1:-1]
    wind_north = coefficients[0][None, None, :, 1:-1, 1:-1]
    wind_east = coefficients[1][None, None, :, 1:-1, 1:-1]
    held = coefficients[2][None, None, :, 1:-1, 1:-1]
    northern = padded[..., 2:, 1:-1]
    southern = padded[..., :-2, 1:-1]
    eastern = padded[..., 1:-1, 2:]
    western = padded[..., 1:-1, :-2]
    mixed = jnp.einsum("vu,wulrn->wvlrn", coupling, centre, precision=HIGHEST)
    drift = -wind_north * (northern - southern) * 0.5 - wind_east * (eastern - western) * 0.5
    spread = KAPPA * (northern + southern + eastern + western - 4.0 * centre)
    return (1.0 - held) * (drift + spread + mixed) - RELAX * held * centre


def adjoint_tendency(padded, coefficients, coupling):
    wind_north = coefficients[0][None, None]
    wind_east = coefficients[1][None, None]
    held = coefficients[2][None, None]
    weighted = (1.0 - held) * padded
    along_north = wind_north * weighted
    along_east = wind_east * weighted
    centre = weighted[..., 1:-1, 1:-1]
    drift = (along_north[..., 2:, 1:-1] - along_north[..., :-2, 1:-1]) * 0.5
    drift = drift + (along_east[..., 1:-1, 2:] - along_east[..., 1:-1, :-2]) * 0.5
    spread = KAPPA * (
        weighted[..., 2:, 1:-1]
        + weighted[..., :-2, 1:-1]
        + weighted[..., 1:-1, 2:]
        + weighted[..., 1:-1, :-2]
        - 4.0 * centre
    )
    mixed = jnp.einsum("uv,wulrn->wvlrn", coupling, centre, precision=HIGHEST)
    return drift + spread + mixed - RELAX * held[..., 1:-1, 1:-1] * padded[..., 1:-1, 1:-1]


def widen(field):
    return jnp.pad(field, ((0, 0), (0, 0), (0, 0), (0, 0), (1, 1)))


def rows_inside(height, reach):
    global_row = (
        lax.axis_index("lat") * height + jnp.arange(height + 2 * reach, dtype=jnp.int32) - reach
    )
    return ((global_row >= 0) & (global_row < height * lax.axis_size("lat"))).astype(jnp.float32)


def advance(field, tendency, coef_pad, coupling, offset):
    height = field.shape[3]
    extended = extended_2(field, (("lat", 3),), 2)
    first = tendency(widen(extended), coef_pad[:, :, offset - 2 : offset + height + 2, :], coupling)
    middle = (extended[..., 1:-1, :] + DT * first) * rows_inside(height, 1)[:, None]
    second = tendency(widen(middle), coef_pad[:, :, offset - 1 : offset + height + 1, :], coupling)
    first = first[..., 1:-1, :]
    return field + 0.5 * DT * (first + second)


def run_steps(field, tendency, coef_pad, coupling, offset):
    for repeat in range(STEPS):
        field = advance(field, tendency, coef_pad, coupling, offset)
    return field


def by_window(increments, wind_lat, wind_lon, boundary, coupling, precision_time):
    offset = 2 * STEPS + 1
    stacked = jnp.stack([wind_lat, wind_lon, boundary.astype(jnp.float32)])
    rimmed = extended_2(stacked, (("lat", 2),), offset)
    coef_pad = jnp.pad(rimmed, ((0, 0), (0, 0), (0, 0), (1, 1)))
    current = run_steps(increments, forward_tendency, coef_pad, coupling, offset)
    previous = from_behind(current, "tm", 1)
    defects = increments - previous
    flattened = defects.reshape(1, -1, defects.shape[4])
    regrouped = jnp.einsum(
        "kj,jcn->kcn",
        precision_time,
        lax.all_to_all(flattened, "tm", split_axis=1, concat_axis=0, tiled=True),
        precision=HIGHEST,
    )
    weighted = lax.all_to_all(regrouped, "tm", split_axis=0, concat_axis=1, tiled=True).reshape(
        defects.shape
    )
    backward = run_steps(weighted, adjoint_tendency, coef_pad, coupling, offset)
    following = from_behind(backward, "tm", -1)
    return weighted - following


def shards(increments, *rest):
    windows, levels = lax.axis_size("tm"), increments.shape[2]
    height, width = increments.shape[3:]
    fits = (
        windows == levels
        and windows & (windows - 1) == 0
        and windows >= 4
        and lax.axis_size("lat") == 2
        and increments.shape[0] == 1
        and height % ROWS == 0
        and width % LANES == 0
        and (2 * STEPS) % ROWS == 0
        and height >= 4 * STEPS
    )
    return (by_level if fits else by_window)(increments, *rest)


def solution(mesh):
    return jax.shard_map(
        shards,
        mesh=mesh,
        in_specs=(
            P(("member", "tm"), None, None, "lat", None),
            P("member", "lat", None),
            P("member", "lat", None),
            P("member", "lat", None),
            P(),
            P(),
        ),
        out_specs=P(("member", "tm"), None, None, "lat", None),
        check_vma=False,
    )
```

```python
import functools

import jax
import jax.numpy as jnp
from jax import lax
from jax.experimental import pallas as pl
from jax.experimental.pallas import tpu as pltpu
from jax.sharding import PartitionSpec as P


STEPS = 4


KAPPA = 0.2
RELAX = 0.5
DT = 0.4
HIGHEST = lax.Precision.HIGHEST
LANES = 128
ROWS = 8
SCALE = 0.5**STEPS


def rolled(values, shift):
    return [pltpu.roll(value, shift, axis=1) for value in values]


def east_of(values, lane):
    moved = rolled(values, LANES - 1)
    count = len(values)
    return [
        jnp.where(lane == LANES - 1, moved[(part + 1) % count], moved[part])
        for part in range(count)
    ]


def west_of(values, lane):
    moved = rolled(values, 1)
    count = len(values)
    return [jnp.where(lane == 0, moved[part - 1], moved[part]) for part in range(count)]


def apply_operator(source, target, coef, coupling, add):
    variables, parts = source.shape[0], source.shape[1]
    tiles = coef.shape[2] // ROWS
    lane = lax.broadcasted_iota(jnp.int32, (ROWS, LANES), 1)
    for tile in range(tiles):
        at = ROWS * (tile + 1)
        here = slice(at, at + ROWS)
        centre = [[source[v, p, here, :] for p in range(parts)] for v in range(variables)]
        east = [east_of(values, lane) for values in centre]
        west = [west_of(values, lane) for values in centre]
        for p in range(parts):
            rows = slice(ROWS * tile, ROWS * (tile + 1))
            to_north, to_south, to_east, to_west = (coef[i, p, rows, :] for i in range(4))
            held = coef[4, p, rows, :] != 0.0
            for v in range(variables):
                mixed = coupling[v][0] * centre[0][p]
                for u in range(1, variables):
                    mixed = mixed + coupling[v][u] * centre[u][p]
                local = jnp.where(held, (1.0 - DT * RELAX) * centre[v][p], mixed)
                lat = (
                    to_north * source[v, p, at + 1 : at + 1 + ROWS, :]
                    + to_south * source[v, p, at - 1 : at - 1 + ROWS, :]
                )
                lon = to_east * east[v][p] + to_west * west[v][p]
                value = local + (lat + lon)
                if add:
                    value = value + target[v, p, here, :]
                target[v, p, here, :] = value


def pitched(rows):
    rows += 2 * ROWS
    return rows + ROWS if rows % (4 * ROWS) == 0 else rows


def clear_rims(rows, *buffers):
    rim = jnp.zeros((ROWS, LANES), jnp.float32)
    for buffer in buffers:
        for v in range(buffer.shape[0]):
            for p in range(buffer.shape[1]):
                buffer[v, p, 0:ROWS, :] = rim
                buffer[v, p, ROWS + rows : 2 * ROWS + rows, :] = rim


def run_window(state, middle, coef, coupling):
    def step(_, carry):
        apply_operator(state, middle, coef, coupling, False)
        apply_operator(middle, state, coef, coupling, True)
        return carry

    lax.fori_loop(0, STEPS, step, 0)


def aligned(start):
    return pl.ds(pl.multiple_of(start, ROWS), ROWS)


def prepare_kernel(own, halo, forward, adjoint, joined, kept):
    side = lax.axis_index("lat")
    reach, height = halo.shape[1], own.shape[1]
    parts = forward.shape[1]
    lane = lax.broadcasted_iota(jnp.int32, (ROWS, LANES), 1)
    for i in range(3):
        for p in range(parts):
            lanes = slice(p * LANES, (p + 1) * LANES)
            for t in range(height // ROWS):
                joined[i, p, aligned(reach * side + ROWS * t), :] = own[
                    i, ROWS * t : ROWS * (t + 1), lanes
                ]
            for t in range(reach // ROWS):
                joined[i, p, aligned(height * (1 - side) + ROWS * t), :] = halo[
                    i, ROWS * t : ROWS * (t + 1), lanes
                ]
    clear_rims(height + reach, kept)
    tiles = (height + reach) // ROWS
    for t in range(tiles):
        rows = slice(ROWS * t, ROWS * (t + 1))
        here = slice(ROWS * (t + 1), ROWS * (t + 2))
        for p in range(parts):
            north, east, held = (joined[i, p, rows, :] for i in range(3))
            free = DT * (1.0 - held)
            values = [
                free * (KAPPA - 0.5 * north),
                free * (KAPPA + 0.5 * north),
                free * (KAPPA - 0.5 * east),
                free * (KAPPA + 0.5 * east),
            ]
            if p == parts - 1:
                values[2] = jnp.where(lane == LANES - 1, 0.0, values[2])
            if p == 0:
                values[3] = jnp.where(lane == 0, 0.0, values[3])
            for i, value in enumerate(values + [held]):
                forward[i, p, rows, :] = value
            for i in range(4):
                kept[i, p, here, :] = values[i]
    for t in range(tiles):
        rows = slice(ROWS * t, ROWS * (t + 1))
        at = ROWS * (t + 1)
        here = slice(at, at + ROWS)
        from_east = east_of([kept[3, p, here, :] for p in range(parts)], lane)
        from_west = west_of([kept[2, p, here, :] for p in range(parts)], lane)
        for p in range(parts):
            joined[0, p, rows, :] = kept[1, p, at + 1 : at + 1 + ROWS, :]
            joined[1, p, rows, :] = kept[0, p, at - 1 : at - 1 + ROWS, :]
            joined[3, p, rows, :] = from_east[p]
            joined[4, p, rows, :] = from_west[p]
    for t in range(adjoint.shape[2] // ROWS):
        rows = slice(ROWS * t, ROWS * (t + 1))
        at = aligned(reach // 2 * side + ROWS * t)
        for p in range(parts):
            for i, j in enumerate((0, 1, 3, 4, 2)):
                adjoint[i, p, rows, :] = joined[j, p, at, :]


def prepare(own, halo):
    _, height, width = own.shape
    reach = halo.shape[1]
    parts = width // LANES
    vmem = pl.BlockSpec(memory_space=pltpu.VMEM)
    return pl.pallas_call(
        prepare_kernel,
        out_shape=(
            jax.ShapeDtypeStruct((5, parts, height + reach, LANES), jnp.float32),
            jax.ShapeDtypeStruct((5, parts, height + reach // 2, LANES), jnp.float32),
        ),
        in_specs=[vmem, vmem],
        out_specs=(vmem, vmem),
        scratch_shapes=[
            pltpu.VMEM((5, parts, height + reach, LANES), jnp.float32),
            pltpu.VMEM((4, parts, pitched(height + reach), LANES), jnp.float32),
        ],
        compiler_params=pltpu.CompilerParams(vmem_limit_bytes=16 * 2**20),
        cost_estimate=pl.CostEstimate(flops=2**20, bytes_accessed=2**20, transcendentals=0),
        name="prepare",
    )(own, halo)


def forward_kernel(masks, skip, first, scalars, precision, coef, halo, *rest):
    count = len(masks)
    pieces, rest = rest[:count], rest[count:]
    if first:
        total, state, middle, initial = rest
        before = None
    else:
        before, total, state, middle, initial = rest
    side = lax.axis_index("lat")
    me = lax.axis_index("tm")
    variables, height = pieces[0].shape[0], pieces[0].shape[1]
    reach = halo.shape[1]
    parts = coef.shape[1]
    windows, inner = total.shape[2:4]
    coupling = [[scalars[v, u] for u in range(variables)] for v in range(variables)]
    clear_rims(height + reach, state, middle)
    for s, piece in enumerate(pieces):
        for v in range(variables):
            for p in range(parts):
                lanes = slice(p * LANES, (p + 1) * LANES)
                for t in range(height // ROWS):
                    state[v, p, aligned(ROWS + reach * side + ROWS * t), :] = piece[
                        v, ROWS * t : ROWS * (t + 1), lanes
                    ]
                for t in range(reach // ROWS):
                    state[v, p, aligned(ROWS + height * (1 - side) + ROWS * t), :] = halo[
                        skip + s * variables + v, ROWS * t : ROWS * (t + 1), lanes
                    ]
        for v in range(variables):
            for p in range(parts):
                for t in range(inner // ROWS):
                    initial[v, p, ROWS * t : ROWS * (t + 1), :] = state[
                        v, p, aligned(ROWS + reach // 2 * side + ROWS * t), :
                    ]
        run_window(state, middle, coef, coupling)
        window = lax.bitwise_xor(me, masks[s])
        later = jnp.minimum(window + 1, windows - 1)
        scale = jnp.where(window + 1 < windows, -SCALE, 0.0)
        of_initial = [precision[k, window] for k in range(windows)]
        of_final = [precision[k, later] for k in range(windows)]
        base = None if first and s == 0 else (total if first or s else before)

        def accumulate(v, carry):
            for p in range(parts):
                for t in range(inner // ROWS):
                    rows = slice(ROWS * t, ROWS * (t + 1))
                    start = initial[v, p, rows, :]
                    end = state[v, p, aligned(ROWS + reach // 2 * side + ROWS * t), :] * scale
                    values = [0.0 if base is None else base[v, p, k, rows, :] for k in range(windows)]
                    values = [
                        value + (of_initial[k] * start + of_final[k] * end)
                        for k, value in enumerate(values)
                    ]
                    for k, value in enumerate(values):
                        total[v, p, k, rows, :] = value
            return carry

        lax.fori_loop(0, variables, accumulate, 0)


def forward(masks, scalars, precision, coef, halo, skip, pieces, before):
    variables, height, width = pieces[0].shape
    parts = width // LANES
    reach = halo.shape[1]
    windows = precision.shape[0]
    first = before is None
    inner = height + reach // 2
    vmem = pl.BlockSpec(memory_space=pltpu.VMEM)
    smem = pl.BlockSpec(memory_space=pltpu.SMEM)
    buffer = pltpu.VMEM((variables, parts, pitched(height + reach), LANES), jnp.float32)
    arguments = [scalars, precision, coef, halo, *pieces] + ([] if first else [before])
    cells = len(pieces) * variables * (height + reach) * width
    return pl.pallas_call(
        functools.partial(forward_kernel, tuple(masks), skip, first),
        out_shape=jax.ShapeDtypeStruct((variables, parts, windows, inner, LANES), jnp.float32),
        in_specs=[smem] * 2 + [vmem] * (len(arguments) - 2),
        out_specs=vmem,
        scratch_shapes=[
            buffer,
            buffer,
            pltpu.VMEM((variables, parts, inner, LANES), jnp.float32),
        ],
        input_output_aliases={} if first else {len(arguments) - 1: 0},
        compiler_params=pltpu.CompilerParams(vmem_limit_bytes=16 * 2**20),
        cost_estimate=pl.CostEstimate(
            flops=cells * 2 * STEPS * 20, bytes_accessed=4 * cells, transcendentals=0
        ),
        name="forward",
    )(*arguments)


def adjoint_kernel(masks, scalars, coef, total, *rest):
    count = len(masks)
    outs, (state, middle) = rest[:count], rest[count:]
    side = lax.axis_index("lat")
    me = lax.axis_index("tm")
    variables, parts, windows, inner = total.shape[:4]
    height = outs[0].shape[1]
    margin = inner - height
    coupling = [[scalars[u, v] for u in range(variables)] for v in range(variables)]
    clear_rims(inner, state, middle)
    for s, out in enumerate(outs):
        window = lax.bitwise_xor(me, masks[s])
        later = jnp.minimum(window + 1, windows - 1)
        present = window + 1 < windows
        for v in range(variables):
            for p in range(parts):
                for t in range(inner // ROWS):
                    value = total[v, p, later, ROWS * t : ROWS * (t + 1), :]
                    state[v, p, ROWS * (t + 1) : ROWS * (t + 2), :] = jnp.where(
                        present, value, 0.0
                    )
        run_window(state, middle, coef, coupling)
        for v in range(variables):
            for p in range(parts):
                for t in range(height // ROWS):
                    mine = total[v, p, window, aligned(margin * side + ROWS * t), :]
                    back = state[v, p, aligned(ROWS + margin * side + ROWS * t), :]
                    out[v, ROWS * t : ROWS * (t + 1), p * LANES : (p + 1) * LANES] = (
                        mine - SCALE * back
                    )


def adjoint(masks, scalars, coef, total, height):
    count = len(masks)
    variables, parts, _, inner = total.shape[:4]
    vmem = pl.BlockSpec(memory_space=pltpu.VMEM)
    smem = pl.BlockSpec(memory_space=pltpu.SMEM)
    buffer = pltpu.VMEM((variables, parts, pitched(inner), LANES), jnp.float32)
    shape = jax.ShapeDtypeStruct((variables, height, parts * LANES), jnp.float32)
    cells = count * variables * inner * parts * LANES
    return pl.pallas_call(
        functools.partial(adjoint_kernel, tuple(masks)),
        out_shape=(shape,) * count,
        in_specs=[smem, vmem, vmem],
        out_specs=(vmem,) * count,
        scratch_shapes=[buffer, buffer],
        compiler_params=pltpu.CompilerParams(vmem_limit_bytes=16 * 2**20),
        cost_estimate=pl.CostEstimate(
            flops=cells * 2 * STEPS * 20, bytes_accessed=4 * cells, transcendentals=0
        ),
        name="adjoint",
    )(scalars, coef, total)


def plan(windows):
    half = windows // 2
    crossing = list(range(half, windows))
    near = list(range(2, half))
    sending = crossing[:1] + near + [1] + crossing[1:]
    working = [[mask] for mask in [0, 1] + crossing[:1] + near + crossing[1:]]
    back = crossing[half // 2 :] + crossing[: half // 2]
    returning = []
    for index, mask in enumerate(back):
        returning += [mask] + (near[index - 2 : index - 1] if index > 1 else [])
    returning += [1, 0]
    return sending, working, returning


def by_level(increments, wind_lat, wind_lon, boundary, coupling, precision_time):
    windows = lax.axis_size("tm")
    me = lax.axis_index("tm")
    side = lax.axis_index("lat")
    height = increments.shape[3]
    reach = 4 * STEPS
    seam = (1 - side) * (height - reach)
    field = increments[0]
    barrier = lax.optimization_barrier

    def level_of(array, index, dim):
        return lax.dynamic_index_in_dim(array, index, dim, keepdims=False)

    def swapped(value, mask):
        return lax.ppermute(value, "tm", [(i, i ^ mask) for i in range(windows)])

    order, forward_groups, adjoint_order = plan(windows)
    pieces = {mask: level_of(field, me ^ mask, 1) for mask in order + [0]}
    for mask in order:
        pieces[mask] = swapped(pieces[mask], mask)
    own = jnp.stack(
        [
            level_of(wind_lat, me, 0),
            level_of(wind_lon, me, 0),
            level_of(boundary, me, 0).astype(jnp.float32),
        ]
    )
    factor = jnp.float32(1.0 - 4.0 * KAPPA * DT)
    scalars = DT * coupling + factor * jnp.eye(coupling.shape[0], dtype=jnp.float32)

    total = coef_forward = None
    halos = {}

    def fetch(values, key):
        rows = [lax.dynamic_slice_in_dim(value, seam, reach, axis=1) for value in values]
        halos[key] = lax.ppermute(jnp.concatenate(rows), "lat", [(0, 1), (1, 0)])

    fetch([own, pieces[0]], 0)
    skip = own.shape[0]
    coef_forward, coef_adjoint = prepare(own, halos[0][:skip])
    for index, group in enumerate(forward_groups):
        if group[0] not in halos:
            held, total = barrier(([pieces[mask] for mask in group], total))
            pieces.update(zip(group, held))
            fetch(held, group[0])
        if index + 1 < len(forward_groups) - 2:
            after = forward_groups[index + 1]
            if total is not None:
                held, total = barrier(([pieces[mask] for mask in after], total))
                pieces.update(zip(after, held))
            fetch([pieces[mask] for mask in after], after[0])
        total = forward(
            group,
            scalars,
            precision_time,
            coef_forward,
            halos[group[0]],
            skip if group == [0] else 0,
            [pieces[mask] for mask in group],
            total,
        )

    gradient = jnp.zeros_like(field)
    for mask in adjoint_order:
        (result,) = adjoint([mask], scalars, coef_adjoint, total, height)
        if mask:
            result = swapped(result, mask)
        gradient = lax.dynamic_update_slice(gradient, result[:, None], (0, me ^ mask, 0, 0))
    return gradient[None]


def extended_2(block, sides, width):
    for axis, dim in sides:
        count = lax.axis_size(axis)
        forward = [(i, i + 1) for i in range(count - 1)]
        backward = [(target, source) for source, target in forward]
        low = lax.ppermute(
            lax.slice_in_dim(block, block.shape[dim] - width, None, axis=dim), axis, forward
        )
        high = lax.ppermute(lax.slice_in_dim(block, 0, width, axis=dim), axis, backward)
        block = jnp.concatenate([low, block, high], axis=dim)
    return block


def from_behind(value, axis, steps):
    count = lax.axis_size(axis)
    initial, last = (max(0, -steps), min(count, count - steps))
    return lax.ppermute(value, axis, [(source, source + steps) for source in range(initial, last)])


def forward_tendency(padded, coefficients, coupling):
    centre = padded[..., 1:-1, 1:-1]
    wind_north = coefficients[0][None, None, :, 1:-1, 1:-1]
    wind_east = coefficients[1][None, None, :, 1:-1, 1:-1]
    held = coefficients[2][None, None, :, 1:-1, 1:-1]
    northern = padded[..., 2:, 1:-1]
    southern = padded[..., :-2, 1:-1]
    eastern = padded[..., 1:-1, 2:]
    western = padded[..., 1:-1, :-2]
    mixed = jnp.einsum("vu,wulrn->wvlrn", coupling, centre, precision=HIGHEST)
    drift = -wind_north * (northern - southern) * 0.5 - wind_east * (eastern - western) * 0.5
    spread = KAPPA * (northern + southern + eastern + western - 4.0 * centre)
    return (1.0 - held) * (drift + spread + mixed) - RELAX * held * centre


def adjoint_tendency(padded, coefficients, coupling):
    wind_north = coefficients[0][None, None]
    wind_east = coefficients[1][None, None]
    held = coefficients[2][None, None]
    weighted = (1.0 - held) * padded
    along_north = wind_north * weighted
    along_east = wind_east * weighted
    centre = weighted[..., 1:-1, 1:-1]
    drift = (along_north[..., 2:, 1:-1] - along_north[..., :-2, 1:-1]) * 0.5
    drift = drift + (along_east[..., 1:-1, 2:] - along_east[..., 1:-1, :-2]) * 0.5
    spread = KAPPA * (
        weighted[..., 2:, 1:-1]
        + weighted[..., :-2, 1:-1]
        + weighted[..., 1:-1, 2:]
        + weighted[..., 1:-1, :-2]
        - 4.0 * centre
    )
    mixed = jnp.einsum("uv,wulrn->wvlrn", coupling, centre, precision=HIGHEST)
    return drift + spread + mixed - RELAX * held[..., 1:-1, 1:-1] * padded[..., 1:-1, 1:-1]


def widen(field):
    return jnp.pad(field, ((0, 0), (0, 0), (0, 0), (0, 0), (1, 1)))


def rows_inside(height, reach):
    global_row = (
        lax.axis_index("lat") * height + jnp.arange(height + 2 * reach, dtype=jnp.int32) - reach
    )
    return ((global_row >= 0) & (global_row < height * lax.axis_size("lat"))).astype(jnp.float32)


def advance(field, tendency, coef_pad, coupling, offset):
    height = field.shape[3]
    extended = extended_2(field, (("lat", 3),), 2)
    first = tendency(widen(extended), coef_pad[:, :, offset - 2 : offset + height + 2, :], coupling)
    middle = (extended[..., 1:-1, :] + DT * first) * rows_inside(height, 1)[:, None]
    second = tendency(widen(middle), coef_pad[:, :, offset - 1 : offset + height + 1, :], coupling)
    first = first[..., 1:-1, :]
    return field + 0.5 * DT * (first + second)


def run_steps(field, tendency, coef_pad, coupling, offset):
    for _ in range(STEPS):
        field = advance(field, tendency, coef_pad, coupling, offset)
    return field


def by_window(increments, wind_lat, wind_lon, boundary, coupling, precision_time):
    offset = 2 * STEPS + 1
    stacked = jnp.stack([wind_lat, wind_lon, boundary.astype(jnp.float32)])
    rimmed = extended_2(stacked, (("lat", 2),), offset)
    coef_pad = jnp.pad(rimmed, ((0, 0), (0, 0), (0, 0), (1, 1)))
    current = run_steps(increments, forward_tendency, coef_pad, coupling, offset)
    previous = from_behind(current, "tm", 1)
    defects = increments - previous
    flattened = defects.reshape(1, -1, defects.shape[4])
    regrouped = jnp.einsum(
        "kj,jcn->kcn",
        precision_time,
        lax.all_to_all(flattened, "tm", split_axis=1, concat_axis=0, tiled=True),
        precision=HIGHEST,
    )
    weighted = lax.all_to_all(regrouped, "tm", split_axis=0, concat_axis=1, tiled=True).reshape(
        defects.shape
    )
    backward = run_steps(weighted, adjoint_tendency, coef_pad, coupling, offset)
    following = from_behind(backward, "tm", -1)
    return weighted - following


def shards(increments, *rest):
    windows, levels = lax.axis_size("tm"), increments.shape[2]
    height, width = increments.shape[3:]
    fits = (
        windows == levels
        and windows & (windows - 1) == 0
        and windows >= 4
        and lax.axis_size("lat") == 2
        and increments.shape[0] == 1
        and height % ROWS == 0
        and width % LANES == 0
        and (2 * STEPS) % ROWS == 0
        and height >= 4 * STEPS
    )
    return (by_level if fits else by_window)(increments, *rest)


def solution(mesh):
    _, _, _ = plan(mesh.shape["tm"])
    return planned(mesh)


def planned(mesh):
    return jax.shard_map(
        shards,
        mesh=mesh,
        in_specs=(
            P(("member", "tm"), None, None, "lat", None),
            P("member", "lat", None),
            P("member", "lat", None),
            P("member", "lat", None),
            P(),
            P(),
        ),
        out_specs=P(("member", "tm"), None, None, "lat", None),
        check_vma=False,
    )
```

```python
import functools

import jax
import jax.numpy as jnp
from jax import lax
from jax.experimental import pallas as pl
from jax.experimental.pallas import tpu as pltpu
from jax.sharding import PartitionSpec as P


STEPS = 4


KAPPA = 0.2
RELAX = 0.5
DT = 0.4
HIGHEST = lax.Precision.HIGHEST
LANES = 128
ROWS = 8
SCALE = 0.5**STEPS


def rolled(values, shift):
    return [pltpu.roll(value, shift, axis=1) for value in values]


def east_of(values, lane):
    moved = rolled(values, LANES - 1)
    count = len(values)
    return [
        jnp.where(lane == LANES - 1, moved[(part + 1) % count], moved[part])
        for part in range(count)
    ]


def west_of(values, lane):
    moved = rolled(values, 1)
    count = len(values)
    return [jnp.where(lane == 0, moved[part - 1], moved[part]) for part in range(count)]


def apply_operator(source, target, coef, mixing, add):
    variables, parts = source.shape[0], source.shape[1]
    tiles = coef.shape[2] // ROWS
    lane = lax.broadcasted_iota(jnp.int32, (ROWS, LANES), 1)
    for tile in range(tiles):
        at = ROWS * (tile + 1)
        here = slice(at, at + ROWS)
        centre = [[source[v, p, here, :] for p in range(parts)] for v in range(variables)]
        east = [east_of(values, lane) for values in centre]
        west = [west_of(values, lane) for values in centre]
        for p in range(parts):
            rows = slice(ROWS * tile, ROWS * (tile + 1))
            to_north, to_south, to_east, to_west = (coef[i, p, rows, :] for i in range(4))
            held = coef[4, p, rows, :] != 0.0
            for v in range(variables):
                mixed = mixing[v, 0] * centre[0][p]
                for u in range(1, variables):
                    mixed = mixed + mixing[v, u] * centre[u][p]
                local = jnp.where(held, (1.0 - DT * RELAX) * centre[v][p], mixed)
                lat = (
                    to_north * source[v, p, at + 1 : at + 1 + ROWS, :]
                    + to_south * source[v, p, at - 1 : at - 1 + ROWS, :]
                )
                lon = to_east * east[v][p] + to_west * west[v][p]
                value = local + (lat + lon)
                if add:
                    value = value + target[v, p, here, :]
                target[v, p, here, :] = value


def pitched(rows):
    rows += 2 * ROWS
    return rows + ROWS if rows % (4 * ROWS) == 0 else rows


def clear_rims(rows, *buffers):
    rim = jnp.zeros((ROWS, LANES), jnp.float32)
    for buffer in buffers:
        for v in range(buffer.shape[0]):
            for p in range(buffer.shape[1]):
                buffer[v, p, 0:ROWS, :] = rim
                buffer[v, p, ROWS + rows : 2 * ROWS + rows, :] = rim


def run_window(state, middle, coef, mixing):
    def step(_, carry):
        apply_operator(state, middle, coef, mixing, False)
        apply_operator(middle, state, coef, mixing, True)
        return carry

    lax.fori_loop(0, STEPS, step, 0)


def aligned(start):
    return pl.ds(pl.multiple_of(start, ROWS), ROWS)


def prepare_kernel(
    coupling, precision, own, halo, forward, adjoint, mixing, weights, joined, kept
):
    side = lax.axis_index("lat")
    variables, windows = coupling.shape[0], precision.shape[0]

    def tile(value):
        return jnp.full((ROWS, LANES), value, jnp.float32)

    for v in range(variables):
        for u in range(variables):
            value = DT * tile(coupling[v, u])
            if u == v:
                value = value + (1.0 - 4.0 * KAPPA * DT)
            mixing[0, v, u] = value
            mixing[1, u, v] = value

    def weigh(j, carry):
        for k in range(windows):
            weights[j, 0, k] = tile(precision[k, j])
            later = tile(precision[k, jnp.minimum(j + 1, windows - 1)])
            weights[j, 1, k] = jnp.where(j + 1 < windows, -SCALE * later, 0.0)
        return carry

    lax.fori_loop(0, windows, weigh, 0)
    reach, height = halo.shape[1], own.shape[1]
    parts = forward.shape[1]
    lane = lax.broadcasted_iota(jnp.int32, (ROWS, LANES), 1)
    for i in range(3):
        for p in range(parts):
            lanes = slice(p * LANES, (p + 1) * LANES)
            for t in range(height // ROWS):
                joined[i, p, aligned(reach * side + ROWS * t), :] = own[
                    i, ROWS * t : ROWS * (t + 1), lanes
                ]
            for t in range(reach // ROWS):
                joined[i, p, aligned(height * (1 - side) + ROWS * t), :] = halo[
                    i, ROWS * t : ROWS * (t + 1), lanes
                ]
    clear_rims(height + reach, kept)
    tiles = (height + reach) // ROWS
    for t in range(tiles):
        rows = slice(ROWS * t, ROWS * (t + 1))
        here = slice(ROWS * (t + 1), ROWS * (t + 2))
        for p in range(parts):
            north, east, held = (joined[i, p, rows, :] for i in range(3))
            free = DT * (1.0 - held)
            values = [
                free * (KAPPA - 0.5 * north),
                free * (KAPPA + 0.5 * north),
                free * (KAPPA - 0.5 * east),
                free * (KAPPA + 0.5 * east),
            ]
            if p == parts - 1:
                values[2] = jnp.where(lane == LANES - 1, 0.0, values[2])
            if p == 0:
                values[3] = jnp.where(lane == 0, 0.0, values[3])
            for i, value in enumerate(values + [held]):
                forward[i, p, rows, :] = value
            for i in range(4):
                kept[i, p, here, :] = values[i]
    for t in range(tiles):
        rows = slice(ROWS * t, ROWS * (t + 1))
        at = ROWS * (t + 1)
        here = slice(at, at + ROWS)
        from_east = east_of([kept[3, p, here, :] for p in range(parts)], lane)
        from_west = west_of([kept[2, p, here, :] for p in range(parts)], lane)
        for p in range(parts):
            joined[0, p, rows, :] = kept[1, p, at + 1 : at + 1 + ROWS, :]
            joined[1, p, rows, :] = kept[0, p, at - 1 : at - 1 + ROWS, :]
            joined[3, p, rows, :] = from_east[p]
            joined[4, p, rows, :] = from_west[p]
    for t in range(adjoint.shape[2] // ROWS):
        rows = slice(ROWS * t, ROWS * (t + 1))
        at = aligned(reach // 2 * side + ROWS * t)
        for p in range(parts):
            for i, j in enumerate((0, 1, 3, 4, 2)):
                adjoint[i, p, rows, :] = joined[j, p, at, :]


def prepare(coupling, precision, own, halo):
    variables, windows = coupling.shape[0], precision.shape[0]
    _, height, width = own.shape
    reach = halo.shape[1]
    parts = width // LANES
    vmem = pl.BlockSpec(memory_space=pltpu.VMEM)
    smem = pl.BlockSpec(memory_space=pltpu.SMEM)
    return pl.pallas_call(
        prepare_kernel,
        out_shape=(
            jax.ShapeDtypeStruct((5, parts, height + reach, LANES), jnp.float32),
            jax.ShapeDtypeStruct((5, parts, height + reach // 2, LANES), jnp.float32),
            jax.ShapeDtypeStruct((2, variables, variables, ROWS, LANES), jnp.float32),
            jax.ShapeDtypeStruct((windows, 2, windows, ROWS, LANES), jnp.float32),
        ),
        in_specs=[smem, smem, vmem, vmem],
        out_specs=(vmem,) * 4,
        scratch_shapes=[
            pltpu.VMEM((5, parts, height + reach, LANES), jnp.float32),
            pltpu.VMEM((4, parts, pitched(height + reach), LANES), jnp.float32),
        ],
        compiler_params=pltpu.CompilerParams(vmem_limit_bytes=16 * 2**20),
        cost_estimate=pl.CostEstimate(flops=2**20, bytes_accessed=2**20, transcendentals=0),
        name="prepare",
    )(coupling, precision, own, halo)


def forward_kernel(masks, skip, first, mixing, weights, coef, halo, *rest):
    count = len(masks)
    pieces, rest = rest[:count], rest[count:]
    if first:
        total, state, middle, initial = rest
        before = None
    else:
        before, total, state, middle, initial = rest
    side = lax.axis_index("lat")
    me = lax.axis_index("tm")
    variables, height = pieces[0].shape[0], pieces[0].shape[1]
    reach = halo.shape[1]
    parts = coef.shape[1]
    windows, inner = total.shape[2:4]
    clear_rims(height + reach, state, middle)
    for s, piece in enumerate(pieces):
        for v in range(variables):
            for p in range(parts):
                lanes = slice(p * LANES, (p + 1) * LANES)
                for t in range(height // ROWS):
                    state[v, p, aligned(ROWS + reach * side + ROWS * t), :] = piece[
                        v, ROWS * t : ROWS * (t + 1), lanes
                    ]
                for t in range(reach // ROWS):
                    state[v, p, aligned(ROWS + height * (1 - side) + ROWS * t), :] = halo[
                        skip + s * variables + v, ROWS * t : ROWS * (t + 1), lanes
                    ]
        for v in range(variables):
            for p in range(parts):
                for t in range(inner // ROWS):
                    initial[v, p, ROWS * t : ROWS * (t + 1), :] = state[
                        v, p, aligned(ROWS + reach // 2 * side + ROWS * t), :
                    ]
        run_window(state, middle, coef, mixing.at[0])
        window = lax.bitwise_xor(me, masks[s])
        base = None if first and s == 0 else (total if first or s else before)

        def accumulate(v, carry):
            for p in range(parts):
                for t in range(inner // ROWS):
                    rows = slice(ROWS * t, ROWS * (t + 1))
                    start = initial[v, p, rows, :]
                    end = state[v, p, aligned(ROWS + reach // 2 * side + ROWS * t), :]
                    values = [0.0 if base is None else base[v, p, k, rows, :] for k in range(windows)]
                    values = [
                        value + (weights[window, 0, k] * start + weights[window, 1, k] * end)
                        for k, value in enumerate(values)
                    ]
                    for k, value in enumerate(values):
                        total[v, p, k, rows, :] = value
            return carry

        lax.fori_loop(0, variables, accumulate, 0)


def forward(masks, mixing, weights, coef, halo, skip, pieces, before):
    variables, height, width = pieces[0].shape
    parts = width // LANES
    reach = halo.shape[1]
    windows = weights.shape[0]
    first = before is None
    inner = height + reach // 2
    vmem = pl.BlockSpec(memory_space=pltpu.VMEM)
    smem = pl.BlockSpec(memory_space=pltpu.SMEM)
    buffer = pltpu.VMEM((variables, parts, pitched(height + reach), LANES), jnp.float32)
    arguments = [mixing, weights, coef, halo, *pieces] + ([] if first else [before])
    cells = len(pieces) * variables * (height + reach) * width
    return pl.pallas_call(
        functools.partial(forward_kernel, tuple(masks), skip, first),
        out_shape=jax.ShapeDtypeStruct((variables, parts, windows, inner, LANES), jnp.float32),
        in_specs=[vmem] * len(arguments),
        out_specs=vmem,
        scratch_shapes=[
            buffer,
            buffer,
            pltpu.VMEM((variables, parts, inner, LANES), jnp.float32),
        ],
        input_output_aliases={} if first else {len(arguments) - 1: 0},
        compiler_params=pltpu.CompilerParams(vmem_limit_bytes=16 * 2**20),
        cost_estimate=pl.CostEstimate(
            flops=cells * 2 * STEPS * 20, bytes_accessed=4 * cells, transcendentals=0
        ),
        name="forward",
    )(*arguments)


def adjoint_kernel(masks, mixing, coef, total, *rest):
    count = len(masks)
    outs, (state, middle) = rest[:count], rest[count:]
    side = lax.axis_index("lat")
    me = lax.axis_index("tm")
    variables, parts, windows, inner = total.shape[:4]
    height = outs[0].shape[1]
    margin = inner - height
    clear_rims(inner, state, middle)
    for s, out in enumerate(outs):
        window = lax.bitwise_xor(me, masks[s])
        later = jnp.minimum(window + 1, windows - 1)
        present = window + 1 < windows
        for v in range(variables):
            for p in range(parts):
                for t in range(inner // ROWS):
                    value = total[v, p, later, ROWS * t : ROWS * (t + 1), :]
                    state[v, p, ROWS * (t + 1) : ROWS * (t + 2), :] = jnp.where(
                        present, value, 0.0
                    )
        run_window(state, middle, coef, mixing.at[1])
        for v in range(variables):
            for p in range(parts):
                for t in range(height // ROWS):
                    mine = total[v, p, window, aligned(margin * side + ROWS * t), :]
                    back = state[v, p, aligned(ROWS + margin * side + ROWS * t), :]
                    out[v, ROWS * t : ROWS * (t + 1), p * LANES : (p + 1) * LANES] = (
                        mine - SCALE * back
                    )


def adjoint(masks, mixing, coef, total, height):
    count = len(masks)
    variables, parts, _, inner = total.shape[:4]
    vmem = pl.BlockSpec(memory_space=pltpu.VMEM)
    smem = pl.BlockSpec(memory_space=pltpu.SMEM)
    buffer = pltpu.VMEM((variables, parts, pitched(inner), LANES), jnp.float32)
    shape = jax.ShapeDtypeStruct((variables, height, parts * LANES), jnp.float32)
    cells = count * variables * inner * parts * LANES
    return pl.pallas_call(
        functools.partial(adjoint_kernel, tuple(masks)),
        out_shape=(shape,) * count,
        in_specs=[vmem] * 3,
        out_specs=(vmem,) * count,
        scratch_shapes=[buffer, buffer],
        compiler_params=pltpu.CompilerParams(vmem_limit_bytes=16 * 2**20),
        cost_estimate=pl.CostEstimate(
            flops=cells * 2 * STEPS * 20, bytes_accessed=4 * cells, transcendentals=0
        ),
        name="adjoint",
    )(mixing, coef, total)


def plan(windows):
    half = windows // 2
    crossing = list(range(half, windows))
    near = list(range(2, half))
    sending = crossing[:1] + near[:1] + [1] + near[1:] + crossing[1:]
    working = [[mask] for mask in [0, 1] + crossing[:1] + near + crossing[1:]]
    back = crossing[half // 2 :] + crossing[: half // 2]
    returning = []
    for index, mask in enumerate(back):
        returning += [mask] + (near[index - 2 : index - 1] if index > 1 else [])
    returning = returning[: half // 2] + [1] + returning[half // 2 :] + [0]
    return sending, working, returning


def by_level(increments, wind_lat, wind_lon, boundary, coupling, precision_time):
    windows = lax.axis_size("tm")
    me = lax.axis_index("tm")
    side = lax.axis_index("lat")
    height = increments.shape[3]
    reach = 4 * STEPS
    seam = (1 - side) * (height - reach)
    field = increments[0]
    barrier = lax.optimization_barrier

    def level_of(array, index, dim):
        return lax.dynamic_index_in_dim(array, index, dim, keepdims=False)

    def swapped(value, mask):
        return lax.ppermute(value, "tm", [(i, i ^ mask) for i in range(windows)])

    order, forward_groups, adjoint_order = plan(windows)
    pieces = {mask: level_of(field, me ^ mask, 1) for mask in order + [0]}
    for mask in order:
        pieces[mask] = swapped(pieces[mask], mask)
    own = jnp.stack(
        [
            level_of(wind_lat, me, 0),
            level_of(wind_lon, me, 0),
            level_of(boundary, me, 0).astype(jnp.float32),
        ]
    )
    total = None
    halos = {}

    def fetch(values, key):
        rows = [lax.dynamic_slice_in_dim(value, seam, reach, axis=1) for value in values]
        halos[key] = lax.ppermute(jnp.concatenate(rows), "lat", [(0, 1), (1, 0)])

    fetch([own, pieces[0]], 0)
    skip = own.shape[0]
    coef_forward, coef_adjoint, mixing, weights = prepare(
        coupling, precision_time, own, halos[0][:skip]
    )
    for index, group in enumerate(forward_groups):
        if group[0] not in halos:
            held, total = barrier(([pieces[mask] for mask in group], total))
            pieces.update(zip(group, held))
            fetch(held, group[0])
        if index + 1 < len(forward_groups) - 2:
            after = forward_groups[index + 1]
            if total is not None:
                held, total = barrier(([pieces[mask] for mask in after], total))
                pieces.update(zip(after, held))
            fetch([pieces[mask] for mask in after], after[0])
        total = forward(
            group,
            mixing,
            weights,
            coef_forward,
            halos[group[0]],
            skip if group == [0] else 0,
            [pieces[mask] for mask in group],
            total,
        )

    results = {}
    for mask in adjoint_order:
        (result,) = adjoint([mask], mixing, coef_adjoint, total, height)
        results[mask] = swapped(result, mask) if mask else result
    gradient = jnp.zeros_like(field)
    last = max(mask for mask in adjoint_order if mask < 3 * windows // 4)
    for mask in [mask for mask in adjoint_order if mask != last] + [last]:
        gradient = lax.dynamic_update_slice(
            gradient, results[mask][:, None], (0, me ^ mask, 0, 0)
        )
    return gradient[None]


def extended_2(block, sides, width):
    for axis, dim in sides:
        count = lax.axis_size(axis)
        forward = [(i, i + 1) for i in range(count - 1)]
        backward = [(target, source) for source, target in forward]
        low = lax.ppermute(
            lax.slice_in_dim(block, block.shape[dim] - width, None, axis=dim), axis, forward
        )
        high = lax.ppermute(lax.slice_in_dim(block, 0, width, axis=dim), axis, backward)
        block = jnp.concatenate([low, block, high], axis=dim)
    return block


def from_behind(value, axis, steps):
    count = lax.axis_size(axis)
    initial, last = (max(0, -steps), min(count, count - steps))
    return lax.ppermute(value, axis, [(source, source + steps) for source in range(initial, last)])


def forward_tendency(padded, coefficients, coupling):
    centre = padded[..., 1:-1, 1:-1]
    wind_north = coefficients[0][None, None, :, 1:-1, 1:-1]
    wind_east = coefficients[1][None, None, :, 1:-1, 1:-1]
    held = coefficients[2][None, None, :, 1:-1, 1:-1]
    northern = padded[..., 2:, 1:-1]
    southern = padded[..., :-2, 1:-1]
    eastern = padded[..., 1:-1, 2:]
    western = padded[..., 1:-1, :-2]
    mixed = jnp.einsum("vu,wulrn->wvlrn", coupling, centre, precision=HIGHEST)
    drift = -wind_north * (northern - southern) * 0.5 - wind_east * (eastern - western) * 0.5
    spread = KAPPA * (northern + southern + eastern + western - 4.0 * centre)
    return (1.0 - held) * (drift + spread + mixed) - RELAX * held * centre


def adjoint_tendency(padded, coefficients, coupling):
    wind_north = coefficients[0][None, None]
    wind_east = coefficients[1][None, None]
    held = coefficients[2][None, None]
    weighted = (1.0 - held) * padded
    along_north = wind_north * weighted
    along_east = wind_east * weighted
    centre = weighted[..., 1:-1, 1:-1]
    drift = (along_north[..., 2:, 1:-1] - along_north[..., :-2, 1:-1]) * 0.5
    drift = drift + (along_east[..., 1:-1, 2:] - along_east[..., 1:-1, :-2]) * 0.5
    spread = KAPPA * (
        weighted[..., 2:, 1:-1]
        + weighted[..., :-2, 1:-1]
        + weighted[..., 1:-1, 2:]
        + weighted[..., 1:-1, :-2]
        - 4.0 * centre
    )
    mixed = jnp.einsum("uv,wulrn->wvlrn", coupling, centre, precision=HIGHEST)
    return drift + spread + mixed - RELAX * held[..., 1:-1, 1:-1] * padded[..., 1:-1, 1:-1]


def widen(field):
    return jnp.pad(field, ((0, 0), (0, 0), (0, 0), (0, 0), (1, 1)))


def rows_inside(height, reach):
    global_row = (
        lax.axis_index("lat") * height + jnp.arange(height + 2 * reach, dtype=jnp.int32) - reach
    )
    return ((global_row >= 0) & (global_row < height * lax.axis_size("lat"))).astype(jnp.float32)


def advance(field, tendency, coef_pad, coupling, offset):
    height = field.shape[3]
    extended = extended_2(field, (("lat", 3),), 2)
    first = tendency(widen(extended), coef_pad[:, :, offset - 2 : offset + height + 2, :], coupling)
    middle = (extended[..., 1:-1, :] + DT * first) * rows_inside(height, 1)[:, None]
    second = tendency(widen(middle), coef_pad[:, :, offset - 1 : offset + height + 1, :], coupling)
    first = first[..., 1:-1, :]
    return field + 0.5 * DT * (first + second)


def run_steps(field, tendency, coef_pad, coupling, offset):
    for _ in range(STEPS):
        field = advance(field, tendency, coef_pad, coupling, offset)
    return field


def by_window(increments, wind_lat, wind_lon, boundary, coupling, precision_time):
    offset = 2 * STEPS + 1
    stacked = jnp.stack([wind_lat, wind_lon, boundary.astype(jnp.float32)])
    rimmed = extended_2(stacked, (("lat", 2),), offset)
    coef_pad = jnp.pad(rimmed, ((0, 0), (0, 0), (0, 0), (1, 1)))
    current = run_steps(increments, forward_tendency, coef_pad, coupling, offset)
    previous = from_behind(current, "tm", 1)
    defects = increments - previous
    flattened = defects.reshape(1, -1, defects.shape[4])
    regrouped = jnp.einsum(
        "kj,jcn->kcn",
        precision_time,
        lax.all_to_all(flattened, "tm", split_axis=1, concat_axis=0, tiled=True),
        precision=HIGHEST,
    )
    weighted = lax.all_to_all(regrouped, "tm", split_axis=0, concat_axis=1, tiled=True).reshape(
        defects.shape
    )
    backward = run_steps(weighted, adjoint_tendency, coef_pad, coupling, offset)
    following = from_behind(backward, "tm", -1)
    return weighted - following


def shards(increments, *rest):
    windows, levels = lax.axis_size("tm"), increments.shape[2]
    height, width = increments.shape[3:]
    fits = (
        windows == levels
        and windows & (windows - 1) == 0
        and windows >= 4
        and lax.axis_size("lat") == 2
        and increments.shape[0] == 1
        and height % ROWS == 0
        and width % LANES == 0
        and (2 * STEPS) % ROWS == 0
        and height >= 4 * STEPS
    )
    return (by_level if fits else by_window)(increments, *rest)


def solution(mesh):
    _, _, _ = plan(mesh.shape["tm"])
    return planned(mesh)


def planned(mesh):
    return jax.shard_map(
        shards,
        mesh=mesh,
        in_specs=(
            P(("member", "tm"), None, None, "lat", None),
            P("member", "lat", None),
            P("member", "lat", None),
            P("member", "lat", None),
            P(),
            P(),
        ),
        out_specs=P(("member", "tm"), None, None, "lat", None),
        check_vma=False,
    )
```
